32 devices in a mesh: gx: 4 (over y, x), gy: 4 (over z), gz: 2 (over core).
Axes of the slice: x: 2, y: 2, z: 4, core: 2. Of those that a mesh axis runs over, the one named last changes fastest.
Arguments:
- densities: float32 [7, 64, 128, 512], P(None, 'gz', 'gy', 'gx'), may hold values from -6 to 6
- residuals: float32 [7, 64, 128, 512], P(None, 'gz', 'gy', 'gx'), may hold values from -320 to 320
Outputs:
- new_density: float32 [64, 128, 512], P('gz', 'gy', 'gx')
- weights: float32 [7], replicated
The draws below stay inside these ranges and needn't reach their ends.
All inputs are finite; a program needn't handle non-finite values.
Results may differ from the reference program's by a relative error of at most 0.000087.
Values sent between devices are 32-bit elements; how exact they have to be, the bound alone decides.
A program may use at most 64 MiB of HBM per device.

```python
import math
import jax
import jax.numpy as jnp
from jax import lax

HIST1 = 7
SWEEPS = 3
NX = 512
NY = 128
NZ = 64


def draw_residuals(key, part):
    keys = jax.random.split(jax.random.fold_in(key, 11), 4)
    base = jnp.clip(jax.random.normal(keys[0], (1, NZ, NY, NX), jnp.float32), -6.0, 6.0)
    zpos = jnp.arange(NZ, dtype=jnp.float32) / NZ
    rows = jnp.exp(jax.random.uniform(keys[3], (1, 1, NY, 1), jnp.float32, 0.0, math.log(3.0)))
    noise = 0.7 * jnp.clip(jax.random.normal(keys[1], (HIST1, NZ, NY, NX), jnp.float32), -6.0, 6.0)
    mixing = jax.random.uniform(keys[2], (HIST1, 1, 1, 1), jnp.float32, 0.5, 1.0)
    ramp = jnp.power(10.0, zpos)
    return (mixing * base + noise) * ramp.reshape(1, NZ, 1, 1) * rows


def levels(own_key, extent, pieces, low, top_value):
    loudness, own = 1.0, jax.random.fold_in(own_key, 6)
    for axis_at, blocks in pieces:
        heights = jnp.exp(jax.random.uniform(jax.random.fold_in(own, axis_at), (blocks,), jnp.float32, low / len(pieces), top_value / len(pieces)))
        loudness = loudness * jnp.repeat(heights, extent[axis_at] // blocks).reshape([-1 if axis == axis_at else 1 for axis in range(len(extent))])
    return loudness


def scatter_about(own_key, dims, spread, bound, shards=(), held_as=jnp.bfloat16):
    array = spread * jax.random.normal(own_key, dims, jnp.float32)
    if shards:
        array = array * levels(own_key, dims, shards, -0.22, 0.18)
    return jnp.clip(array, -bound, bound).astype(held_as)


def setup_inputs(seed: int = 0) -> dict:
    seeds = jax.random.split(jax.random.key(seed), 3)
    return {
        "densities": scatter_about(seeds[0], (HIST1, NZ, NY, NX), 1.0, 6.0, ((1, 2), (2, 4), (3, 4)), jnp.float32),
        "residuals": draw_residuals(jax.random.fold_in(seeds[2], 71), 0),
    }


shift_value = 0.15
mix_amount = 0.7

def sweep_weights():
    diag_value = 6.0 + shift_value
    upper = (shift_value + 12.0) / diag_value
    lower = upper / 3.0
    return [1.0 / ((upper + lower) / 2.0 + (upper - lower) / 2.0 * math.cos(math.pi * (2 * k - 1) / (2 * SWEEPS))) for k in range(1, SWEEPS + 1)]

def neighbours(field):
    total = jnp.roll(field, 1, 0) + jnp.roll(field, -1, 0)
    total = total + jnp.roll(field, 1, 1) + jnp.roll(field, -1, 1)
    return total + jnp.roll(field, 1, 2) + jnp.roll(field, -1, 2)

def reference(densities, residuals):
    flat = residuals.reshape(HIST1, -1)
    gram = jnp.dot(flat.astype(jnp.float32), flat.T.astype(jnp.float32), precision=lax.Precision.HIGHEST, preferred_element_type=jnp.float32)
    factor = jnp.linalg.cholesky(gram)
    ones_column = jnp.ones((HIST1, 1), jnp.float32)
    middle = lax.linalg.triangular_solve(factor, ones_column, left_side=True, lower=True)
    solved = lax.linalg.triangular_solve(factor, middle, left_side=True, lower=True, transpose_a=True)[:, 0]
    weights = solved / jnp.sum(solved)
    blended = jnp.tensordot(weights, densities, axes=1, precision=lax.Precision.HIGHEST)
    combined = jnp.tensordot(weights, residuals, axes=1, precision=lax.Precision.HIGHEST)
    diag_value = 6.0 + shift_value
    omegas = sweep_weights()
    rhs = 6.0 * combined - neighbours(combined)
    iterate = omegas[0] * rhs / diag_value
    for position in range(1, SWEEPS):
        iterate = iterate + omegas[position] * (rhs - diag_value * iterate + neighbours(iterate)) / diag_value
    return (blended + mix_amount * iterate, weights)
```

```python
import functools
import math

import jax
import jax.numpy as jnp
from jax import lax
from jax.experimental import pallas as pl
from jax.experimental.pallas import tpu as pltpu
from jax.sharding import PartitionSpec as P

MESH = pl.DeviceIdType.MESH
SWEEPS = 3
SUB = 8
shift_value = 0.15
mix_amount = 0.7
AXES = ("gx", "gy", "gz")


def sweep_weights():
    diag_value = 6.0 + shift_value
    upper = (shift_value + 12.0) / diag_value
    lower = upper / 3.0
    return [
        1.0
        / (
            (upper + lower) / 2.0
            + (upper - lower) / 2.0 * math.cos(math.pi * (2 * k - 1) / (2 * SWEEPS))
        )
        for k in range(1, SWEEPS + 1)
    ]


def kernel(
    counts, dims, chunks,
    res, den, out, wout,
    held, dens, slots, comb, side, rhs_a, rhs_b, it_a, it_b, zland, packs, landed,
    in_sem, den_sem, gsend, grecv, zsend, zrecv, ysend, yrecv, xsend, xrecv,
):
    count, nz, ny, nx = dims
    cx, cy, cz = counts
    total_devices = cx * cy * cz
    zp = nz + SUB
    h = SWEEPS
    ix, iy, iz = (lax.axis_index(a) for a in AXES)
    me = (ix * cy + iy) * cz + iz

    def coords(flat):
        return (flat // (cy * cz), lax.rem(flat // cz, cy), lax.rem(flat, cz))

    def near(dx, dy, dz):
        return (
            lax.rem(ix + dx + cx, cx),
            lax.rem(iy + dy + cy, cy),
            lax.rem(iz + dz + cz, cz),
        )

    per = nz // chunks
    loads = []
    for c in range(chunks):
        part = pl.ds(c * per, per)
        cp = pltpu.make_async_copy(res.at[:, part], held.at[:, part], in_sem.at[c])
        cp.start()
        loads.append(cp)
    den_load = pltpu.make_async_copy(den, dens, den_sem)
    den_load.start()

    barrier = pltpu.get_barrier_semaphore()

    @pl.loop(1, total_devices)
    def _(k):
        pl.semaphore_signal(
            barrier, inc=1, device_id=coords(lax.rem(me + k, total_devices)), device_id_type=MESH
        )

    pl.semaphore_wait(barrier, total_devices - 1)

    pairs = [(i, j) for i in range(count) for j in range(i, count)]
    tiles = ny // SUB
    accs = tuple(jnp.zeros((SUB, nx), jnp.float32) for _ in pairs)
    for c in range(chunks):
        loads[c].wait()

        def gram_step(z, accs):
            accs = list(accs)
            for t in range(tiles):
                v = [held[i, z, t * SUB:(t + 1) * SUB, :] for i in range(count)]
                for p, (i, j) in enumerate(pairs):
                    accs[p] = accs[p] + v[i] * v[j]
            return tuple(accs)

        accs = lax.fori_loop(c * per, (c + 1) * per, gram_step, accs)
    lane = lax.broadcasted_iota(jnp.int32, (SUB, nx), 1)
    packed = jnp.zeros((SUB, nx), jnp.float32)
    for p in range(len(pairs)):
        packed = jnp.where(lane == p, jnp.sum(accs[p], axis=1, keepdims=True), packed)
    slots[pl.ds(me, 1)] = jnp.sum(packed, axis=0, keepdims=True).reshape(1, 1, nx)

    def gram_copy(k, slot, target):
        return pltpu.make_async_remote_copy(
            src_ref=slots.at[me],
            dst_ref=slots.at[slot],
            send_sem=gsend.at[k],
            recv_sem=grecv.at[slot],
            device_id=coords(target),
            device_id_type=MESH,
        )

    @pl.loop(1, total_devices)
    def _(k):
        gram_copy(k, me, lax.rem(me + k, total_devices)).start()

    @pl.loop(1, total_devices)
    def _(k):
        other = lax.rem(me + k, total_devices)
        gram_copy(k, other, other).wait_recv()

    total = jnp.sum(slots[...], axis=0)

    g = {}
    for p, (i, j) in enumerate(pairs):
        g[i, j] = jnp.broadcast_to(total[:, p:p + 1], (SUB, nx))
    b = [jnp.ones((SUB, nx), jnp.float32) for _ in range(count)]
    inv = []
    for k in range(count):
        inv.append(1.0 / g[k, k])
        for i in range(k + 1, count):
            f = g[k, i] * inv[k]
            for j in range(i, count):
                g[i, j] = g[i, j] - f * g[k, j]
            b[i] = b[i] - f * b[k]
    solved = [None] * count
    for k in reversed(range(count)):
        s = b[k]
        for j in range(k + 1, count):
            s = s - g[k, j] * solved[j]
        solved[k] = s * inv[k]
    norm = solved[0]
    for k in range(1, count):
        norm = norm + solved[k]
    weights = [s / norm for s in solved]
    row = jnp.zeros((SUB, nx), jnp.float32)
    for k in range(count):
        row = jnp.where(lane == k, weights[k], row)
    wout[...] = row[0:1, :count]

    flat = comb.reshape((ny + 2 * h) * zp, nx)

    @pl.loop(0, nz)
    def _(z):
        for t in range(tiles):
            s = weights[0] * held[0, z, t * SUB:(t + 1) * SUB, :]
            for i in range(1, count):
                s = s + weights[i] * held[i, z, t * SUB:(t + 1) * SUB, :]
            flat[pl.ds((h + t * SUB) * zp + z, SUB, stride=zp), :] = s

    own = pl.ds(h, ny)
    zcopies = []
    for k, (start, dz) in enumerate(((0, -1), (nz - SUB, 1))):
        cp = pltpu.make_async_remote_copy(
            src_ref=comb.at[own, pl.ds(start, SUB)],
            dst_ref=zland.at[k],
            send_sem=zsend.at[k],
            recv_sem=zrecv.at[k],
            device_id=near(0, 0, dz),
            device_id_type=MESH,
        )
        cp.start()
        zcopies.append(cp)
    for cp in zcopies:
        cp.wait()
    sub = lax.broadcasted_iota(jnp.int32, (SUB, nx), 0)

    @pl.loop(0, ny, unroll=4)
    def _(y):
        comb[h + y, nz:zp, :] = jnp.where(sub < SUB // 2, zland[0, y], zland[1, y])

    ycopies = []
    for k, (start, dest, dy) in enumerate(((h, ny + h, -1), (ny, 0, 1))):
        cp = pltpu.make_async_remote_copy(
            src_ref=comb.at[pl.ds(start, h)],
            dst_ref=comb.at[pl.ds(dest, h)],
            send_sem=ysend.at[k],
            recv_sem=yrecv.at[k],
            device_id=near(0, dy, 0),
            device_id_type=MESH,
        )
        cp.start()
        ycopies.append(cp)

    group = lane // h

    @pl.loop(0, zp // SUB)
    def _(zt):
        rows = pl.ds(pl.multiple_of(zt * SUB, SUB), SUB)
        head = jnp.zeros((SUB, nx), jnp.float32)
        tail = jnp.zeros((SUB, nx), jnp.float32)
        for y in range(ny):
            v = comb[h + y, rows, :]
            here = group == y
            head = jnp.where(here, pltpu.roll(v, (h * y) % nx, 1), head)
            tail = jnp.where(here, pltpu.roll(v, (h * y + h) % nx, 1), tail)
        packs[0, rows, :] = head
        packs[1, rows, :] = tail

    xcopies = []
    for k, dx in enumerate((-1, 1)):
        for dy in (0, -1, 1):
            cp = pltpu.make_async_remote_copy(
                src_ref=packs.at[k],
                dst_ref=landed.at[k, 1 - dy],
                send_sem=xsend.at[k, 1 - dy],
                recv_sem=xrecv.at[k, 1 - dy],
                device_id=near(dx, dy, 0),
                device_id_type=MESH,
            )
            cp.start()
            xcopies.append(cp)

    den_load.wait()

    @pl.loop(0, nz)
    def _(z):
        for t in range(tiles):
            s = weights[0] * dens[0, z, t * SUB:(t + 1) * SUB, :]
            for i in range(1, count):
                s = s + weights[i] * dens[i, z, t * SUB:(t + 1) * SUB, :]
            out[z, t * SUB:(t + 1) * SUB, :] = s

    for cp in xcopies:
        cp.wait()

    @pl.loop(0, zp // SUB)
    def _(zt):
        rows = pl.ds(pl.multiple_of(zt * SUB, SUB), SUB)
        for e in range(ny + 2 * h):
            if e < h:
                slot, y = 0, ny - h + e
            elif e < ny + h:
                slot, y = 1, e - h
            else:
                slot, y = 2, e - h - ny
            head = pltpu.roll(landed[0, slot, rows, :], (-h * y) % nx, 1)
            tail = pltpu.roll(landed[1, slot, rows, :], (nx - h - h * y) % nx, 1)
            side[e, rows, :] = jnp.where(lane < nx // 2, head, tail)

    for cp in ycopies:
        cp.wait()

    wide = lax.broadcasted_iota(jnp.int32, (zp, nx), 1)
    first, last = wide == 0, wide == nx - 1

    def around(fa, fb, e, both):
        a, s = fa[e], fb[e]
        ra, rs = pltpu.roll(a, 1, 1), pltpu.roll(s, 1, 1)
        la, ls = pltpu.roll(a, nx - 1, 1), pltpu.roll(s, nx - 1, 1)
        na = jnp.where(first, rs, ra) + jnp.where(last, ls, la)
        na = na + (pltpu.roll(a, 1, 0) + pltpu.roll(a, zp - 1, 0))
        na = na + (fa[e - 1] + fa[e + 1])
        if not both:
            return a, na
        ns = jnp.where(first, ra, rs) + jnp.where(last, la, ls)
        ns = ns + (pltpu.roll(s, 1, 0) + pltpu.roll(s, zp - 1, 0))
        ns = ns + (fb[e - 1] + fb[e + 1])
        return a, na, s, ns

    diag_value = 6.0 + shift_value
    w1, w2, w3 = sweep_weights()
    alpha = ((1.0 - w2) * w1 + w2) / diag_value
    beta = w1 * w2 / (diag_value * diag_value)

    @pl.loop(1, ny + 2 * h - 1)
    def _(e):
        a, na, s, ns = around(comb, side, e, True)
        rhs_a[e] = 6.0 * a - na
        rhs_b[e] = 6.0 * s - ns

    @pl.loop(2, ny + 2 * h - 2)
    def _(e):
        a, na, s, ns = around(rhs_a, rhs_b, e, True)
        it_a[e] = alpha * a + beta * na
        it_b[e] = alpha * s + beta * ns

    out_flat = out.reshape(nz * ny, nx)

    @pl.loop(3, ny + 2 * h - 3)
    def _(e):
        a, na = around(it_a, it_b, e, False)
        u = (mix_amount * (1.0 - w3)) * a + (mix_amount * w3 / diag_value) * (rhs_a[e] + na)
        for zt in range(nz // SUB):
            rows = pl.ds(zt * SUB * ny + (e - h), SUB, stride=ny)
            out_flat[rows, :] = out_flat[rows, :] + u[zt * SUB:(zt + 1) * SUB, :]

    @pl.loop(1, total_devices)
    def _(k):
        gram_copy(k, me, lax.rem(me + k, total_devices)).wait_send()


def on_device(counts, densities, residuals):
    dims = residuals.shape
    count, nz, ny, nx = dims
    h = SWEEPS
    zp = nz + SUB
    n = counts[0] * counts[1] * counts[2]
    chunks = 4
    field = pltpu.VMEM((ny + 2 * h, zp, nx), jnp.float32)
    dma = pltpu.SemaphoreType.DMA
    any_spec = pl.BlockSpec(memory_space=pl.ANY)
    vmem = pl.BlockSpec(memory_space=pltpu.VMEM)
    new_density, weights = pl.pallas_call(
        functools.partial(kernel, counts, dims, chunks),
        out_shape=(
            jax.ShapeDtypeStruct((nz, ny, nx), jnp.float32),
            jax.ShapeDtypeStruct((1, count), jnp.float32),
        ),
        in_specs=[any_spec, any_spec],
        out_specs=(vmem, vmem),
        scratch_shapes=[
            pltpu.VMEM(dims, jnp.float32),
            pltpu.VMEM(dims, jnp.float32),
            pltpu.VMEM((n, 1, nx), jnp.float32),
            field, field, field, field, field, field,
            pltpu.VMEM((2, ny, SUB, nx), jnp.float32),
            pltpu.VMEM((2, zp, nx), jnp.float32),
            pltpu.VMEM((2, 3, zp, nx), jnp.float32),
            dma((chunks,)), dma(()), dma((n,)), dma((n,)),
            dma((2,)), dma((2,)), dma((2,)), dma((2,)), dma((2, 3)), dma((2, 3)),
        ],
        compiler_params=pltpu.CompilerParams(
            collective_id=0, has_side_effects=True, vmem_limit_bytes=61 * 1024 * 1024
        ),
    )(residuals, densities)
    return new_density, weights.reshape(count)


def solution(mesh):
    counts = tuple(mesh.shape[a] for a in AXES)
    placed = (P(None, "gz", "gy", "gx"), P(None, "gz", "gy", "gx"))
    return jax.shard_map(
        functools.partial(on_device, counts),
        mesh=mesh,
        in_specs=placed,
        out_specs=(P("gz", "gy", "gx"), P()),
        check_vma=False,
    )
```

```python
import functools
import math

import jax
import jax.numpy as jnp
from jax import lax
from jax.experimental import pallas as pl
from jax.experimental.pallas import tpu as pltpu
from jax.sharding import PartitionSpec as P

MESH = pl.DeviceIdType.MESH
SWEEPS = 3
SUB = 8
UNROLL = 2
shift_value = 0.15
mix_amount = 0.7
AXES = ("gx", "gy", "gz")


def sweep_weights():
    diag_value = 6.0 + shift_value
    upper = (shift_value + 12.0) / diag_value
    lower = upper / 3.0
    return [
        1.0
        / (
            (upper + lower) / 2.0
            + (upper - lower) / 2.0 * math.cos(math.pi * (2 * k - 1) / (2 * SWEEPS))
        )
        for k in range(1, SWEEPS + 1)
    ]


def kernel(
    counts, dims, chunks,
    res, den, out, wout,
    held, dens, slots, comb, side, rhs_a, rhs_b, it_a, it_b, packs, landed, cpacks, clanded,
    in_sem, den_sem, gsend, grecv, zsend, zrecv, ysend, yrecv, xsend, xrecv, csend, crecv,
):
    count, nz, ny, nx = dims
    cx, cy, cz = counts
    total_devices = cx * cy * cz
    zp = nz + SUB
    h = SWEEPS
    ix, iy, iz = (lax.axis_index(a) for a in AXES)
    me = (ix * cy + iy) * cz + iz

    def coords(flat):
        return (flat // (cy * cz), lax.rem(flat // cz, cy), lax.rem(flat, cz))

    def near(dx, dy, dz):
        return (
            lax.rem(ix + dx + cx, cx),
            lax.rem(iy + dy + cy, cy),
            lax.rem(iz + dz + cz, cz),
        )

    per = nz // chunks
    loads = []
    for c in range(chunks):
        cp = pltpu.make_async_copy(
            res.at[:, pl.ds(c * per, per)], held.at[:, pl.ds(h + c * per, per)], in_sem.at[c]
        )
        cp.start()
        loads.append(cp)
    den_load = pltpu.make_async_copy(den, dens, den_sem)
    den_load.start()

    barrier = pltpu.get_barrier_semaphore()

    @pl.loop(1, total_devices)
    def _(k):
        pl.semaphore_signal(
            barrier, inc=1, device_id=coords(lax.rem(me + k, total_devices)), device_id_type=MESH
        )

    @pl.loop(h, ny + h)
    def _(y):
        comb[y, nz:zp, :] = jnp.zeros((SUB, nx), jnp.float32)

    pairs = [(i, j) for i in range(count) for j in range(i, count)]
    tiles = ny // SUB
    accs = tuple(jnp.zeros((SUB, nx), jnp.float32) for _ in pairs)
    for c in range(chunks):
        loads[c].wait()

        def gram_step(z, accs):
            accs = list(accs)
            for t in range(tiles):
                v = [held[i, z, t * SUB:(t + 1) * SUB, :] for i in range(count)]
                for p, (i, j) in enumerate(pairs):
                    accs[p] = accs[p] + v[i] * v[j]
            return tuple(accs)

        accs = lax.fori_loop(h + c * per, h + (c + 1) * per, gram_step, accs)
    lane = lax.broadcasted_iota(jnp.int32, (SUB, nx), 1)
    packed = jnp.zeros((SUB, nx), jnp.float32)
    for p in range(len(pairs)):
        packed = jnp.where(lane == p, jnp.sum(accs[p], axis=1, keepdims=True), packed)
    slots[pl.ds(me, 1)] = jnp.sum(packed, axis=0, keepdims=True).reshape(1, 1, nx)

    pl.semaphore_wait(barrier, total_devices - 1)

    def gram_copy(k, slot, target):
        return pltpu.make_async_remote_copy(
            src_ref=slots.at[me],
            dst_ref=slots.at[slot],
            send_sem=gsend.at[k],
            recv_sem=grecv.at[slot],
            device_id=coords(target),
            device_id_type=MESH,
        )

    @pl.loop(1, total_devices)
    def _(k):
        gram_copy(k, me, lax.rem(me + k, total_devices)).start()

    zcopies = []
    for k, (start, dest, dz) in enumerate(((h, nz + h, -1), (nz, 0, 1))):
        cp = pltpu.make_async_remote_copy(
            src_ref=held.at[:, pl.ds(start, h)],
            dst_ref=held.at[:, pl.ds(dest, h)],
            send_sem=zsend.at[k],
            recv_sem=zrecv.at[k],
            device_id=near(0, 0, dz),
            device_id_type=MESH,
        )
        cp.start()
        zcopies.append(cp)

    @pl.loop(1, total_devices)
    def _(k):
        other = lax.rem(me + k, total_devices)
        gram_copy(k, other, other).wait_recv()

    total = jnp.sum(slots[...], axis=0)

    g = {}
    for p, (i, j) in enumerate(pairs):
        g[i, j] = jnp.broadcast_to(total[:, p:p + 1], (SUB, nx))
    b = [jnp.ones((SUB, nx), jnp.float32) for _ in range(count)]
    inv = []
    for k in range(count):
        inv.append(1.0 / g[k, k])
        for i in range(k + 1, count):
            f = g[k, i] * inv[k]
            for j in range(i, count):
                g[i, j] = g[i, j] - f * g[k, j]
            b[i] = b[i] - f * b[k]
    solved = [None] * count
    for k in reversed(range(count)):
        s = b[k]
        for j in range(k + 1, count):
            s = s - g[k, j] * solved[j]
        solved[k] = s * inv[k]
    norm = solved[0]
    for k in range(1, count):
        norm = norm + solved[k]
    weights = [s / norm for s in solved]
    row = jnp.zeros((SUB, nx), jnp.float32)
    for k in range(count):
        row = jnp.where(lane == k, weights[k], row)
    wout[...] = row[0:1, :count]

    flat = comb.reshape((ny + 2 * h) * zp, nx)

    def combine(z, row):
        for t in range(tiles):
            s = weights[0] * held[0, z, t * SUB:(t + 1) * SUB, :]
            for i in range(1, count):
                s = s + weights[i] * held[i, z, t * SUB:(t + 1) * SUB, :]
            flat[pl.ds((h + t * SUB) * zp + row, SUB, stride=zp), :] = s

    @pl.loop(0, nz)
    def _(z):
        combine(z + h, z)

    for cp in zcopies:
        cp.wait()
    for j in range(h):
        combine(j, zp - h + j)
        combine(nz + h + j, nz + j)

    ycopies = []
    for k, (start, dest, dy) in enumerate(((h, ny + h, -1), (ny, 0, 1))):
        cp = pltpu.make_async_remote_copy(
            src_ref=comb.at[pl.ds(start, h)],
            dst_ref=comb.at[pl.ds(dest, h)],
            send_sem=ysend.at[k],
            recv_sem=yrecv.at[k],
            device_id=near(0, dy, 0),
            device_id_type=MESH,
        )
        cp.start()
        ycopies.append(cp)

    group = lane // h

    @pl.loop(0, zp // SUB)
    def _(zt):
        rows = pl.ds(pl.multiple_of(zt * SUB, SUB), SUB)
        head = jnp.zeros((SUB, nx), jnp.float32)
        tail = jnp.zeros((SUB, nx), jnp.float32)
        for y in range(ny):
            v = comb[h + y, rows, :]
            here = group == y
            head = jnp.where(here, pltpu.roll(v, (h * y) % nx, 1), head)
            tail = jnp.where(here, pltpu.roll(v, (h * y + h) % nx, 1), tail)
        packs[0, rows, :] = head
        packs[1, rows, :] = tail

    xcopies = []
    for k, dx in enumerate((-1, 1)):
        cp = pltpu.make_async_remote_copy(
            src_ref=packs.at[k],
            dst_ref=landed.at[k],
            send_sem=xsend.at[k],
            recv_sem=xrecv.at[k],
            device_id=near(dx, 0, 0),
            device_id_type=MESH,
        )
        cp.start()
        xcopies.append(cp)
    span = h * h
    corner_group = lane // span
    for k, dx in enumerate((-1, 1)):
        for q, dy in enumerate((1, -1)):
            first_lane = h * (ny - h) if dy > 0 else 0
            corner = jnp.zeros((SUB, nx), jnp.float32)
            for zt in range(zp // SUB):
                v = packs[k, zt * SUB:(zt + 1) * SUB, :]
                v = pltpu.roll(v, (span * zt - first_lane) % nx, 1)
                corner = jnp.where(corner_group == zt, v, corner)
            cpacks[k, q] = corner
            cp = pltpu.make_async_remote_copy(
                src_ref=cpacks.at[k, q],
                dst_ref=clanded.at[k, q],
                send_sem=csend.at[k, q],
                recv_sem=crecv.at[k, q],
                device_id=near(dx, dy, 0),
                device_id_type=MESH,
            )
            cp.start()
            xcopies.append(cp)

    den_load.wait()

    @pl.loop(0, nz)
    def _(z):
        for t in range(tiles):
            s = weights[0] * dens[0, z, t * SUB:(t + 1) * SUB, :]
            for i in range(1, count):
                s = s + weights[i] * dens[i, z, t * SUB:(t + 1) * SUB, :]
            out[z, t * SUB:(t + 1) * SUB, :] = s

    for cp in xcopies:
        cp.wait()

    left = lane < nx // 2

    @pl.loop(0, zp // SUB)
    def _(zt):
        rows = pl.ds(pl.multiple_of(zt * SUB, SUB), SUB)
        for y in range(ny):
            head = pltpu.roll(landed[0, rows, :], (-h * y) % nx, 1)
            tail = pltpu.roll(landed[1, rows, :], (nx - h - h * y) % nx, 1)
            side[h + y, rows, :] = jnp.where(left, head, tail)

    for q, base in ((0, 0), (1, ny + h)):
        for zt in range(zp // SUB):
            for r in range(h):
                at = span * zt + h * r
                head = pltpu.roll(clanded[0, q], (-at) % nx, 1)
                tail = pltpu.roll(clanded[1, q], (nx - h - at) % nx, 1)
                side[base + r, zt * SUB:(zt + 1) * SUB, :] = jnp.where(left, head, tail)

    for cp in ycopies:
        cp.wait()

    wide = lax.broadcasted_iota(jnp.int32, (zp, nx), 1)
    first, last = wide == 0, wide == nx - 1

    def around(fa, fb, e, both):
        a, s = fa[e], fb[e]
        ra, rs = pltpu.roll(a, 1, 1), pltpu.roll(s, 1, 1)
        la, ls = pltpu.roll(a, nx - 1, 1), pltpu.roll(s, nx - 1, 1)
        na = jnp.where(first, rs, ra) + jnp.where(last, ls, la)
        na = na + (pltpu.roll(a, 1, 0) + pltpu.roll(a, zp - 1, 0))
        na = na + (fa[e - 1] + fa[e + 1])
        if not both:
            return a, na
        ns = jnp.where(first, ra, rs) + jnp.where(last, la, ls)
        ns = ns + (pltpu.roll(s, 1, 0) + pltpu.roll(s, zp - 1, 0))
        ns = ns + (fb[e - 1] + fb[e + 1])
        return a, na, s, ns

    diag_value = 6.0 + shift_value
    w1, w2, w3 = sweep_weights()
    alpha = ((1.0 - w2) * w1 + w2) / diag_value
    beta = w1 * w2 / (diag_value * diag_value)

    def planes(start, stop, unroll):
        unroll = unroll if (stop - start) % unroll == 0 else 1

        def wrap(body):
            @pl.loop(0, (stop - start) // unroll)
            def _(it):
                for r in range(unroll):
                    body(start + it * unroll + r)

        return wrap

    @planes(1, ny + 2 * h - 1, UNROLL)
    def _(e):
        a, na, s, ns = around(comb, side, e, True)
        rhs_a[e] = 6.0 * a - na
        rhs_b[e] = 6.0 * s - ns

    @planes(2, ny + 2 * h - 2, UNROLL)
    def _(e):
        a, na, s, ns = around(rhs_a, rhs_b, e, True)
        it_a[e] = alpha * a + beta * na
        it_b[e] = alpha * s + beta * ns

    out_flat = out.reshape(nz * ny, nx)

    @planes(3, ny + 2 * h - 3, UNROLL)
    def _(e):
        a, na = around(it_a, it_b, e, False)
        u = (mix_amount * (1.0 - w3)) * a + (mix_amount * w3 / diag_value) * (rhs_a[e] + na)
        for zt in range(nz // SUB):
            rows = pl.ds(zt * SUB * ny + (e - h), SUB, stride=ny)
            out_flat[rows, :] = out_flat[rows, :] + u[zt * SUB:(zt + 1) * SUB, :]

    @pl.loop(1, total_devices)
    def _(k):
        gram_copy(k, me, lax.rem(me + k, total_devices)).wait_send()


def hand_over(mixed, weights, out, wout, sem):
    cp = pltpu.make_async_copy(mixed, out, sem)
    cp.start()
    wout[...] = weights[...]
    cp.wait()


def on_device(counts, densities, residuals):
    dims = residuals.shape
    count, nz, ny, nx = dims
    h = SWEEPS
    zp = nz + SUB
    n = counts[0] * counts[1] * counts[2]
    chunks = 4
    field = pltpu.VMEM((ny + 2 * h, zp, nx), jnp.float32)
    dma = pltpu.SemaphoreType.DMA
    any_spec = pl.BlockSpec(memory_space=pl.ANY)
    vmem = pl.BlockSpec(memory_space=pltpu.VMEM)
    new_density, weights = pl.pallas_call(
        functools.partial(kernel, counts, dims, chunks),
        out_shape=(
            pltpu.VMEM((nz, ny, nx), jnp.float32),
            pltpu.VMEM((1, count), jnp.float32),
        ),
        in_specs=[any_spec, any_spec],
        out_specs=(vmem, vmem),
        scratch_shapes=[
            pltpu.VMEM((count, nz + 2 * h, ny, nx), jnp.float32),
            pltpu.VMEM(dims, jnp.float32),
            pltpu.VMEM((n, 1, nx), jnp.float32),
            field, field, field, field, field, field,
            pltpu.VMEM((2, zp, nx), jnp.float32),
            pltpu.VMEM((2, zp, nx), jnp.float32),
            pltpu.VMEM((2, 2, SUB, nx), jnp.float32),
            pltpu.VMEM((2, 2, SUB, nx), jnp.float32),
            dma((chunks,)), dma(()), dma((n,)), dma((n,)),
            dma((2,)), dma((2,)), dma((2,)), dma((2,)), dma((2,)), dma((2,)), dma((2, 2)), dma((2, 2)),
        ],
        compiler_params=pltpu.CompilerParams(
            collective_id=0, has_side_effects=True, vmem_limit_bytes=61 * 1024 * 1024
        ),
    )(residuals, densities)
    new_density, weights = pl.pallas_call(
        hand_over,
        out_shape=(
            jax.ShapeDtypeStruct((nz, ny, nx), jnp.float32),
            jax.ShapeDtypeStruct((1, count), jnp.float32),
        ),
        in_specs=[vmem, vmem],
        out_specs=(any_spec, vmem),
        scratch_shapes=[dma(())],
        compiler_params=pltpu.CompilerParams(vmem_limit_bytes=4 * 1024 * 1024),
    )(new_density, weights)
    return new_density, weights.reshape(count)


def solution(mesh):
    counts = tuple(mesh.shape[a] for a in AXES)
    placed = (P(None, "gz", "gy", "gx"), P(None, "gz", "gy", "gx"))
    return jax.shard_map(
        functools.partial(on_device, counts),
        mesh=mesh,
        in_specs=placed,
        out_specs=(P("gz", "gy", "gx"), P()),
        check_vma=False,
    )
```

```python
import functools
import math

import jax
import jax.numpy as jnp
from jax import lax
from jax.experimental import pallas as pl
from jax.experimental.pallas import tpu as pltpu
from jax.sharding import PartitionSpec as P

MESH = pl.DeviceIdType.MESH
SWEEPS = 3
SUB = 8
UNROLL = 4
DEEP = 16
shift_value = 0.15
mix_amount = 0.7
AXES = ("gx", "gy", "gz")


def sweep_weights():
    diag_value = 6.0 + shift_value
    upper = (shift_value + 12.0) / diag_value
    lower = upper / 3.0
    return [
        1.0
        / (
            (upper + lower) / 2.0
            + (upper - lower) / 2.0 * math.cos(math.pi * (2 * k - 1) / (2 * SWEEPS))
        )
        for k in range(1, SWEEPS + 1)
    ]


def kernel(
    counts, dims, chunks,
    res, den, out, wout,
    held, dens, slots, comb, rhs_a, it_a, strip, rhs_s, it_s, packs, landed, cfirst, clast,
    in_sem, den_sem, gsend, grecv, zsend, zrecv, ysend, yrecv, xsend, xrecv, csend, crecv,
):
    count, nz, ny, nx = dims
    cx, cy, cz = counts
    total_devices = cx * cy * cz
    zp = nz + SUB
    h = SWEEPS
    ix, iy, iz = (lax.axis_index(a) for a in AXES)
    me = (ix * cy + iy) * cz + iz

    def near(dx, dy, dz):
        return (
            lax.rem(ix + dx + cx, cx),
            lax.rem(iy + dy + cy, cy),
            lax.rem(iz + dz + cz, cz),
        )

    per = nz // chunks
    loads = []
    for c in range(chunks):
        cp = pltpu.make_async_copy(
            res.at[:, pl.ds(c * per, per)], held.at[:, pl.ds(h + c * per, per)], in_sem.at[c]
        )
        cp.start()
        loads.append(cp)
    den_load = pltpu.make_async_copy(den, dens, den_sem)
    den_load.start()

    barrier = pltpu.get_barrier_semaphore()

    offsets = [
        (dx, dy, dz) for dx in range(cx) for dy in range(cy) for dz in range(cz) if dx or dy or dz
    ]
    offsets.sort(key=lambda o: -sum(min(d, c - d) for d, c in zip(o, counts)))
    gx = [lax.rem(ix + d, cx) for d in range(cx)]
    gy = [lax.rem(iy + d, cy) for d in range(cy)]
    gz = [lax.rem(iz + d, cz) for d in range(cz)]
    for dx, dy, dz in offsets:
        pl.semaphore_signal(
            barrier, inc=1, device_id=(gx[dx], gy[dy], gz[dz]), device_id_type=MESH
        )

    @pl.loop(h, ny + h)
    def _(y):
        comb[y, nz:zp, :] = jnp.zeros((SUB, nx), jnp.float32)

    pairs = [(i, j) for i in range(count) for j in range(i, count)]
    tiles = ny // SUB
    accs = tuple(jnp.zeros((SUB, nx), jnp.float32) for _ in pairs)
    for c in range(chunks):
        loads[c].wait()

        def gram_step(z, accs):
            accs = list(accs)
            for t in range(tiles):
                v = [held[i, z, t * SUB:(t + 1) * SUB, :] for i in range(count)]
                for p, (i, j) in enumerate(pairs):
                    accs[p] = accs[p] + v[i] * v[j]
            return tuple(accs)

        accs = lax.fori_loop(h + c * per, h + (c + 1) * per, gram_step, accs)
    lane = lax.broadcasted_iota(jnp.int32, (SUB, nx), 1)
    packed = jnp.zeros((SUB, nx), jnp.float32)
    for p in range(len(pairs)):
        packed = jnp.where(lane == p, jnp.sum(accs[p], axis=1, keepdims=True), packed)
    slots[pl.ds(me, 1)] = jnp.sum(packed, axis=0, keepdims=True).reshape(1, 1, nx)

    pl.semaphore_wait(barrier, total_devices - 1)

    def gram_copy(k, slot):
        dx, dy, dz = offsets[k]
        return pltpu.make_async_remote_copy(
            src_ref=slots.at[me],
            dst_ref=slots.at[slot],
            send_sem=gsend.at[k],
            recv_sem=grecv.at[k],
            device_id=(gx[dx], gy[dy], gz[dz]),
            device_id_type=MESH,
        )

    for k in range(len(offsets)):
        gram_copy(k, me).start()

    zcopies = []
    for k, (start, dest, dz) in enumerate(((h, nz + h, -1), (nz, 0, 1))):
        cp = pltpu.make_async_remote_copy(
            src_ref=held.at[:, pl.ds(start, h)],
            dst_ref=held.at[:, pl.ds(dest, h)],
            send_sem=zsend.at[k],
            recv_sem=zrecv.at[k],
            device_id=near(0, 0, dz),
            device_id_type=MESH,
        )
        cp.start()
        zcopies.append(cp)

    for k, (dx, dy, dz) in enumerate(offsets):
        source = (gx[-dx % cx] * cy + gy[-dy % cy]) * cz + gz[-dz % cz]
        gram_copy(k, source).wait_recv()

    total = jnp.sum(slots[...], axis=0)

    g = {}
    for p, (i, j) in enumerate(pairs):
        g[i, j] = jnp.broadcast_to(total[:, p:p + 1], (SUB, nx))
    b = [jnp.ones((SUB, nx), jnp.float32) for _ in range(count)]
    inv = []
    for k in range(count):
        inv.append(1.0 / g[k, k])
        for i in range(k + 1, count):
            f = g[k, i] * inv[k]
            for j in range(i, count):
                g[i, j] = g[i, j] - f * g[k, j]
            b[i] = b[i] - f * b[k]
    solved = [None] * count
    for k in reversed(range(count)):
        s = b[k]
        for j in range(k + 1, count):
            s = s - g[k, j] * solved[j]
        solved[k] = s * inv[k]
    norm = solved[0]
    for k in range(1, count):
        norm = norm + solved[k]
    weights = [s / norm for s in solved]
    row = jnp.zeros((SUB, nx), jnp.float32)
    for k in range(count):
        row = jnp.where(lane == k, weights[k], row)
    wout[...] = row[0:1, :count]

    flat = comb.reshape((ny + 2 * h) * zp, nx)

    def combine(z, row):
        for t in range(tiles):
            s = weights[0] * held[0, z, t * SUB:(t + 1) * SUB, :]
            for i in range(1, count):
                s = s + weights[i] * held[i, z, t * SUB:(t + 1) * SUB, :]
            flat[pl.ds((h + t * SUB) * zp + row, SUB, stride=zp), :] = s

    @pl.loop(0, nz)
    def _(z):
        combine(z + h, z)

    for cp in zcopies:
        cp.wait()
    for j in range(h):
        combine(j, zp - h + j)
        combine(nz + h + j, nz + j)

    ycopies = []
    for k, (start, dest, dy) in enumerate(((h, ny + h, -1), (ny, 0, 1))):
        cp = pltpu.make_async_remote_copy(
            src_ref=comb.at[pl.ds(start, h)],
            dst_ref=comb.at[pl.ds(dest, h)],
            send_sem=ysend.at[k],
            recv_sem=yrecv.at[k],
            device_id=near(0, dy, 0),
            device_id_type=MESH,
        )
        cp.start()
        ycopies.append(cp)

    ztiles = zp // SUB
    width = 6 * h
    group = lane // width
    inner = lane - width * group
    at_left = inner < 3 * h

    def own_strip(e):
        total = jnp.zeros((SUB, nx), jnp.float32)
        for zt in range(ztiles):
            v = comb[e, zt * SUB:(zt + 1) * SUB, :]
            near_left = pltpu.roll(v, (width * zt + h) % nx, 1)
            near_right = pltpu.roll(v, (width * zt + 5 * h) % nx, 1)
            total = jnp.where(group == zt, jnp.where(at_left, near_left, near_right), total)
        strip[e] = total

    def planes(start, stop, unroll):
        steps = (stop - start) // unroll

        def wrap(body):
            @pl.loop(0, steps)
            def _(it):
                for r in range(unroll):
                    body(start + it * unroll + r)

            for e in range(start + steps * unroll, stop):
                body(e)
            return body

        return wrap

    planes(h, ny + h, 8)(own_strip)

    each = width // h
    place = inner // h
    for m in range(packs.shape[1]):
        head = jnp.zeros((SUB, nx), jnp.float32)
        tail = jnp.zeros((SUB, nx), jnp.float32)
        for q in range(min(each, ny - m * each)):
            v = strip[h + m * each + q]
            head = jnp.where(place == q, pltpu.roll(v, (h * q - h) % nx, 1), head)
            tail = jnp.where(place == q, pltpu.roll(v, (h * q - 4 * h) % nx, 1), tail)
        packs[0, m] = head
        packs[1, m] = tail

    low = (ny - h) // each
    xcopies = []

    def send_x(source, target, send_sem, recv_sem, dx, dy):
        cp = pltpu.make_async_remote_copy(
            src_ref=source,
            dst_ref=target,
            send_sem=send_sem,
            recv_sem=recv_sem,
            device_id=near(dx, dy, 0),
            device_id_type=MESH,
        )
        cp.start()
        xcopies.append(cp)

    for k, dx in enumerate((-1, 1)):
        send_x(
            packs.at[k, pl.ds(low, clast.shape[1])], clast.at[k],
            csend.at[k, 0], crecv.at[k, 0], dx, 1,
        )
        send_x(
            packs.at[k, pl.ds(0, cfirst.shape[1])], cfirst.at[k],
            csend.at[k, 1], crecv.at[k, 1], dx, -1,
        )
    for k, dx in enumerate((-1, 1)):
        send_x(packs.at[k], landed.at[k], xsend.at[k], xrecv.at[k], dx, 0)

    den_load.wait()

    @pl.loop(0, nz)
    def _(z):
        for t in range(tiles):
            s = weights[0] * dens[0, z, t * SUB:(t + 1) * SUB, :]
            for i in range(1, count):
                s = s + weights[i] * dens[i, z, t * SUB:(t + 1) * SUB, :]
            out[z, t * SUB:(t + 1) * SUB, :] = s

    def around(f, e):
        v = f[e]
        total = pltpu.roll(v, 1, 1) + pltpu.roll(v, nx - 1, 1)
        total = total + (pltpu.roll(v, 1, 0) + pltpu.roll(v, zp - 1, 0))
        return v, total + (f[e - 1] + f[e + 1])

    diag_value = 6.0 + shift_value
    w1, w2, w3 = sweep_weights()
    alpha = ((1.0 - w2) * w1 + w2) / diag_value
    beta = w1 * w2 / (diag_value * diag_value)

    def first_pass(e):
        v, total = around(comb, e)
        rhs_a[e] = 6.0 * v - total

    planes(h + 1, ny + h - 1, UNROLL)(first_pass)

    def second_pass(e):
        v, total = around(rhs_a, e)
        it_a[e] = alpha * v + beta * total

    planes(h + 2, ny + h - 2, UNROLL)(second_pass)

    out_flat = out.reshape(nz * ny, nx)
    edge = (lane < h) | (lane >= nx - h)

    def last_step(v, total, r):
        return (mix_amount * (1.0 - w3)) * v + (mix_amount * w3 / diag_value) * (r + total)

    def third_pass(e):
        v, total = around(it_a, e)
        u = last_step(v, total, rhs_a[e])
        for zt in range(nz // SUB):
            rows = pl.ds(zt * SUB * ny + (e - h), SUB, stride=ny)
            part = u[zt * SUB:(zt + 1) * SUB, :]
            out_flat[rows, :] = out_flat[rows, :] + jnp.where(edge, 0.0, part)

    planes(h + 3, ny + h - 3, UNROLL)(third_pass)

    for cp in ycopies:
        cp.wait()

    for e in (*range(h), *range(ny + h, ny + 2 * h)):
        own_strip(e)
    for e in (*range(1, h + 1), *range(ny + h - 1, ny + 2 * h - 1)):
        first_pass(e)
    for e in (*range(2, h + 2), *range(ny + h - 2, ny + 2 * h - 2)):
        second_pass(e)
    for e in (*range(h, h + 3), *range(ny + h - 3, ny + h)):
        third_pass(e)

    for cp in xcopies:
        cp.wait()

    for e in range(ny + 2 * h):
        if e < h:
            ref, y, m0 = clast, ny - h + e, low
        elif e < ny + h:
            ref, y, m0 = landed, e - h, 0
        else:
            ref, y, m0 = cfirst, e - h - ny, 0
        m, q = y // each - m0, y % each
        head = pltpu.roll(ref[0, m], (5 * h - h * q) % nx, 1)
        tail = pltpu.roll(ref[1, m], (-h * q) % nx, 1)
        strip[e] = jnp.where(inner < h, tail, jnp.where(inner >= 5 * h, head, strip[e]))

    sub = lax.broadcasted_iota(jnp.int32, (SUB, nx), 0)
    wrap_by = (ztiles - 1) * width

    def around_strip(f, e):
        v = f[e]
        total = pltpu.roll(v, 1, 1) + pltpu.roll(v, nx - 1, 1)
        below = pltpu.roll(v, 1, 0)
        carried = jnp.where(
            group == 0, pltpu.roll(below, nx - wrap_by, 1), pltpu.roll(below, width, 1)
        )
        total = total + jnp.where(sub == 0, carried, below)
        above = pltpu.roll(v, SUB - 1, 0)
        carried = jnp.where(
            group == ztiles - 1, pltpu.roll(above, wrap_by, 1), pltpu.roll(above, nx - width, 1)
        )
        total = total + jnp.where(sub == SUB - 1, carried, above)
        return v, total + (f[e - 1] + f[e + 1])

    @planes(1, ny + 2 * h - 1, DEEP)
    def _(e):
        v, total = around_strip(strip, e)
        rhs_s[e] = 6.0 * v - total

    @planes(2, ny + 2 * h - 2, DEEP)
    def _(e):
        v, total = around_strip(rhs_s, e)
        it_s[e] = alpha * v + beta * total

    @planes(h, ny + h, DEEP)
    def _(e):
        v, total = around_strip(it_s, e)
        u = last_step(v, total, rhs_s[e])
        for zt in range(nz // SUB):
            rows = pl.ds(zt * SUB * ny + (e - h), SUB, stride=ny)
            from_left = pltpu.roll(u, (-(width * zt + h)) % nx, 1)
            from_right = pltpu.roll(u, (-5 * h - width * zt) % nx, 1)
            part = jnp.where(lane < nx // 2, from_left, from_right)
            out_flat[rows, :] = out_flat[rows, :] + jnp.where(edge, part, 0.0)

    for k in range(len(offsets)):
        gram_copy(k, me).wait_send()


def hand_over(mixed, weights, out, wout, sem):
    cp = pltpu.make_async_copy(mixed, out, sem)
    cp.start()
    wout[...] = weights[...]
    cp.wait()


def on_device(counts, densities, residuals):
    dims = residuals.shape
    count, nz, ny, nx = dims
    h = SWEEPS
    zp = nz + SUB
    n = counts[0] * counts[1] * counts[2]
    chunks = 4
    field = pltpu.VMEM((ny + 2 * h, zp, nx), jnp.float32)
    strips = pltpu.VMEM((ny + 2 * h, SUB, nx), jnp.float32)
    each = 6
    messages = pl.cdiv(ny, each)
    dma = pltpu.SemaphoreType.DMA

    def faces(blocks):
        return pltpu.VMEM((2, blocks, SUB, nx), jnp.float32)

    any_spec = pl.BlockSpec(memory_space=pl.ANY)
    vmem = pl.BlockSpec(memory_space=pltpu.VMEM)
    new_density, weights = pl.pallas_call(
        functools.partial(kernel, counts, dims, chunks),
        out_shape=(
            pltpu.VMEM((nz, ny, nx), jnp.float32),
            pltpu.VMEM((1, count), jnp.float32),
        ),
        in_specs=[any_spec, any_spec],
        out_specs=(vmem, vmem),
        scratch_shapes=[
            pltpu.VMEM((count, nz + 2 * h, ny, nx), jnp.float32),
            pltpu.VMEM(dims, jnp.float32),
            pltpu.VMEM((n, 1, nx), jnp.float32),
            field, field, field, strips, strips, strips,
            faces(messages),
            faces(messages),
            faces(pl.cdiv(h, each)),
            faces(messages - (ny - h) // each),
            dma((chunks,)), dma(()), dma((n,)), dma((n,)),
            dma((2,)), dma((2,)), dma((2,)), dma((2,)), dma((2,)), dma((2,)), dma((2, 2)), dma((2, 2)),
        ],
        compiler_params=pltpu.CompilerParams(
            collective_id=0, has_side_effects=True, vmem_limit_bytes=61 * 1024 * 1024
        ),
    )(residuals, densities)
    new_density, weights = pl.pallas_call(
        hand_over,
        out_shape=(
            jax.ShapeDtypeStruct((nz, ny, nx), jnp.float32),
            jax.ShapeDtypeStruct((1, count), jnp.float32),
        ),
        in_specs=[vmem, vmem],
        out_specs=(any_spec, vmem),
        scratch_shapes=[dma(())],
        compiler_params=pltpu.CompilerParams(vmem_limit_bytes=4 * 1024 * 1024),
    )(new_density, weights)
    return new_density, weights.reshape(count)


def solution(mesh):
    counts = tuple(mesh.shape[a] for a in AXES)
    placed = (P(None, "gz", "gy", "gx"), P(None, "gz", "gy", "gx"))
    return jax.shard_map(
        functools.partial(on_device, counts),
        mesh=mesh,
        in_specs=placed,
        out_specs=(P("gz", "gy", "gx"), P()),
        check_vma=False,
    )
```

```python
import functools
import math

import jax
import jax.numpy as jnp
from jax import lax
from jax.experimental import pallas as pl
from jax.experimental.pallas import tpu as pltpu
from jax.sharding import PartitionSpec as P

MESH = pl.DeviceIdType.MESH
SWEEPS = 3
SUB = 8
UNROLL = 4
DEEP = 16
shift_value = 0.15
mix_amount = 0.7
AXES = ("gx", "gy", "gz")


def sweep_weights():
    diag_value = 6.0 + shift_value
    upper = (shift_value + 12.0) / diag_value
    lower = upper / 3.0
    return [
        1.0
        / (
            (upper + lower) / 2.0
            + (upper - lower) / 2.0 * math.cos(math.pi * (2 * k - 1) / (2 * SWEEPS))
        )
        for k in range(1, SWEEPS + 1)
    ]


def kernel(
    counts, dims, chunks,
    res, den, out, wout,
    held, dens, slots, comb, rhs_a, it_a, final, faces, strip, rhs_s, it_s, packs, landed, cfirst, clast,
    in_sem, den_sem, gsend, grecv, zsend, zrecv, ysend, yrecv, xsend, xrecv, csend, crecv,
):
    count, nz, ny, nx = dims
    cx, cy, cz = counts
    total_devices = cx * cy * cz
    zp = nz + SUB
    h = SWEEPS
    ix, iy, iz = (lax.axis_index(a) for a in AXES)
    me = (ix * cy + iy) * cz + iz

    def near(dx, dy, dz):
        return (
            lax.rem(ix + dx + cx, cx),
            lax.rem(iy + dy + cy, cy),
            lax.rem(iz + dz + cz, cz),
        )

    per = nz // chunks
    loads = []
    for c in range(chunks):
        cp = pltpu.make_async_copy(
            res.at[:, pl.ds(c * per, per)], held.at[:, pl.ds(h + c * per, per)], in_sem.at[c]
        )
        cp.start()
        loads.append(cp)
    den_load = pltpu.make_async_copy(den, dens, den_sem)
    den_load.start()

    barrier = pltpu.get_barrier_semaphore()

    offsets = [
        (dx, dy, dz) for dx in range(cx) for dy in range(cy) for dz in range(cz) if dx or dy or dz
    ]
    offsets.sort(key=lambda o: -sum(min(d, c - d) for d, c in zip(o, counts)))
    gx = [lax.rem(ix + d, cx) for d in range(cx)]
    gy = [lax.rem(iy + d, cy) for d in range(cy)]
    gz = [lax.rem(iz + d, cz) for d in range(cz)]
    for dx, dy, dz in offsets:
        pl.semaphore_signal(
            barrier, inc=1, device_id=(gx[dx], gy[dy], gz[dz]), device_id_type=MESH
        )

    @pl.loop(h, ny + h)
    def _(y):
        comb[y, nz:zp, :] = jnp.zeros((SUB, nx), jnp.float32)

    pairs = [(i, j) for i in range(count) for j in range(i, count)]
    tiles = ny // SUB
    accs = tuple(jnp.zeros((SUB, nx), jnp.float32) for _ in pairs)
    for c in range(chunks):
        loads[c].wait()

        def gram_step(z, accs):
            accs = list(accs)
            for t in range(tiles):
                v = [held[i, z, t * SUB:(t + 1) * SUB, :] for i in range(count)]
                for p, (i, j) in enumerate(pairs):
                    accs[p] = accs[p] + v[i] * v[j]
            return tuple(accs)

        accs = lax.fori_loop(h + c * per, h + (c + 1) * per, gram_step, accs)
    lane = lax.broadcasted_iota(jnp.int32, (SUB, nx), 1)
    packed = jnp.zeros((SUB, nx), jnp.float32)
    for p in range(len(pairs)):
        packed = jnp.where(lane == p, jnp.sum(accs[p], axis=1, keepdims=True), packed)
    slots[pl.ds(me, 1)] = jnp.sum(packed, axis=0, keepdims=True).reshape(1, 1, nx)

    pl.semaphore_wait(barrier, total_devices - 1)

    def gram_copy(k, slot):
        dx, dy, dz = offsets[k]
        return pltpu.make_async_remote_copy(
            src_ref=slots.at[me],
            dst_ref=slots.at[slot],
            send_sem=gsend.at[k],
            recv_sem=grecv.at[k],
            device_id=(gx[dx], gy[dy], gz[dz]),
            device_id_type=MESH,
        )

    for k in range(len(offsets)):
        gram_copy(k, me).start()

    zcopies = []
    for k, (start, dest, dz) in enumerate(((h, nz + h, -1), (nz, 0, 1))):
        cp = pltpu.make_async_remote_copy(
            src_ref=held.at[:, pl.ds(start, h)],
            dst_ref=held.at[:, pl.ds(dest, h)],
            send_sem=zsend.at[k],
            recv_sem=zrecv.at[k],
            device_id=near(0, 0, dz),
            device_id_type=MESH,
        )
        cp.start()
        zcopies.append(cp)

    for k, (dx, dy, dz) in enumerate(offsets):
        source = (gx[-dx % cx] * cy + gy[-dy % cy]) * cz + gz[-dz % cz]
        gram_copy(k, source).wait_recv()

    total = jnp.sum(slots[...], axis=0)

    g = {}
    for p, (i, j) in enumerate(pairs):
        g[i, j] = jnp.broadcast_to(total[:, p:p + 1], (SUB, nx))
    b = [jnp.ones((SUB, nx), jnp.float32) for _ in range(count)]
    inv = []
    for k in range(count):
        inv.append(1.0 / g[k, k])
        for i in range(k + 1, count):
            f = g[k, i] * inv[k]
            for j in range(i, count):
                g[i, j] = g[i, j] - f * g[k, j]
            b[i] = b[i] - f * b[k]
    solved = [None] * count
    for k in reversed(range(count)):
        s = b[k]
        for j in range(k + 1, count):
            s = s - g[k, j] * solved[j]
        solved[k] = s * inv[k]
    norm = solved[0]
    for k in range(1, count):
        norm = norm + solved[k]
    weights = [s / norm for s in solved]
    row = jnp.zeros((SUB, nx), jnp.float32)
    for k in range(count):
        row = jnp.where(lane == k, weights[k], row)
    wout[...] = row[0:1, :count]

    flat = comb.reshape((ny + 2 * h) * zp, nx)

    def combine(z, row):
        for t in range(tiles):
            s = weights[0] * held[0, z, t * SUB:(t + 1) * SUB, :]
            for i in range(1, count):
                s = s + weights[i] * held[i, z, t * SUB:(t + 1) * SUB, :]
            flat[pl.ds((h + t * SUB) * zp + row, SUB, stride=zp), :] = s

    @pl.loop(0, nz)
    def _(z):
        combine(z + h, z)

    for cp in zcopies:
        cp.wait()
    for j in range(h):
        combine(j, zp - h + j)
        combine(nz + h + j, nz + j)

    ztiles = zp // SUB
    width = 6 * h
    group = lane // width
    inner = lane - width * group
    at_left = inner < 3 * h

    def own_strip(e):
        total = jnp.zeros((SUB, nx), jnp.float32)
        for zt in range(ztiles):
            v = comb[e, zt * SUB:(zt + 1) * SUB, :]
            near_left = pltpu.roll(v, (width * zt + h) % nx, 1)
            near_right = pltpu.roll(v, (width * zt + 5 * h) % nx, 1)
            total = jnp.where(group == zt, jnp.where(at_left, near_left, near_right), total)
        strip[e] = total

    def planes(start, stop, unroll):
        steps = (stop - start) // unroll

        def wrap(body):
            @pl.loop(0, steps)
            def _(it):
                for r in range(unroll):
                    body(start + it * unroll + r)

            for e in range(start + steps * unroll, stop):
                body(e)
            return body

        return wrap

    planes(h, ny + h, 8)(own_strip)

    each = width // h
    place = inner // h
    for m in range(packs.shape[1]):
        head = jnp.zeros((SUB, nx), jnp.float32)
        tail = jnp.zeros((SUB, nx), jnp.float32)
        for q in range(min(each, ny - m * each)):
            v = strip[h + m * each + q]
            head = jnp.where(place == q, pltpu.roll(v, (h * q - h) % nx, 1), head)
            tail = jnp.where(place == q, pltpu.roll(v, (h * q - 4 * h) % nx, 1), tail)
        packs[0, m] = head
        packs[1, m] = tail

    low = (ny - h) // each
    xcopies = []

    def send_x(source, target, send_sem, recv_sem, dx, dy):
        cp = pltpu.make_async_remote_copy(
            src_ref=source,
            dst_ref=target,
            send_sem=send_sem,
            recv_sem=recv_sem,
            device_id=near(dx, dy, 0),
            device_id_type=MESH,
        )
        cp.start()
        xcopies.append(cp)

    for k, dx in enumerate((-1, 1)):
        send_x(
            packs.at[k, pl.ds(low, clast.shape[1])], clast.at[k],
            csend.at[k, 0], crecv.at[k, 0], dx, 1,
        )
        send_x(
            packs.at[k, pl.ds(0, cfirst.shape[1])], cfirst.at[k],
            csend.at[k, 1], crecv.at[k, 1], dx, -1,
        )
    for k, dx in enumerate((-1, 1)):
        send_x(packs.at[k], landed.at[k], xsend.at[k], xrecv.at[k], dx, 0)

    ycopies = []
    for k, (start, dest, dy) in enumerate(((h, ny + h, -1), (ny, 0, 1))):
        cp = pltpu.make_async_remote_copy(
            src_ref=comb.at[pl.ds(start, h)],
            dst_ref=comb.at[pl.ds(dest, h)],
            send_sem=ysend.at[k],
            recv_sem=yrecv.at[k],
            device_id=near(0, dy, 0),
            device_id_type=MESH,
        )
        cp.start()
        ycopies.append(cp)

    den_load.wait()

    @pl.loop(0, nz)
    def _(z):
        for t in range(tiles):
            s = weights[0] * dens[0, z, t * SUB:(t + 1) * SUB, :]
            for i in range(1, count):
                s = s + weights[i] * dens[i, z, t * SUB:(t + 1) * SUB, :]
            out[z, t * SUB:(t + 1) * SUB, :] = s

    def around(f, e):
        v = f[e]
        total = pltpu.roll(v, 1, 1) + pltpu.roll(v, nx - 1, 1)
        total = total + (pltpu.roll(v, 1, 0) + pltpu.roll(v, zp - 1, 0))
        return v, total + (f[e - 1] + f[e + 1])

    diag_value = 6.0 + shift_value
    w1, w2, w3 = sweep_weights()
    alpha = ((1.0 - w2) * w1 + w2) / diag_value
    beta = w1 * w2 / (diag_value * diag_value)

    def first_pass(e):
        v, total = around(comb, e)
        rhs_a[e] = 6.0 * v - total

    planes(h + 1, ny + h - 1, UNROLL)(first_pass)

    def second_pass(e):
        v, total = around(rhs_a, e)
        it_a[e] = alpha * v + beta * total

    planes(h + 2, ny + h - 2, UNROLL)(second_pass)

    edge = (lane < h) | (lane >= nx - h)

    def last_step(v, total, r):
        return (mix_amount * (1.0 - w3)) * v + (mix_amount * w3 / diag_value) * (r + total)

    def third_pass(e):
        v, total = around(it_a, e)
        u = last_step(v, total, rhs_a[e])
        for zt in range(nz // SUB):
            rows = slice(zt * SUB, (zt + 1) * SUB)
            final[e, rows, :] = u[rows, :]

    planes(h + 3, ny + h - 3, UNROLL)(third_pass)

    for cp in ycopies:
        cp.wait()

    for e in (*range(h), *range(ny + h, ny + 2 * h)):
        own_strip(e)
    for e in (*range(1, h + 1), *range(ny + h - 1, ny + 2 * h - 1)):
        first_pass(e)
    for e in (*range(2, h + 2), *range(ny + h - 2, ny + 2 * h - 2)):
        second_pass(e)
    for e in (*range(h, h + 3), *range(ny + h - 3, ny + h)):
        third_pass(e)

    for cp in xcopies:
        cp.wait()

    for e in range(ny + 2 * h):
        if e < h:
            ref, y, m0 = clast, ny - h + e, low
        elif e < ny + h:
            ref, y, m0 = landed, e - h, 0
        else:
            ref, y, m0 = cfirst, e - h - ny, 0
        m, q = y // each - m0, y % each
        head = pltpu.roll(ref[0, m], (5 * h - h * q) % nx, 1)
        tail = pltpu.roll(ref[1, m], (-h * q) % nx, 1)
        strip[e] = jnp.where(inner < h, tail, jnp.where(inner >= 5 * h, head, strip[e]))

    sub = lax.broadcasted_iota(jnp.int32, (SUB, nx), 0)
    wrap_by = (ztiles - 1) * width

    def around_strip(f, e):
        v = f[e]
        total = pltpu.roll(v, 1, 1) + pltpu.roll(v, nx - 1, 1)
        below = pltpu.roll(v, 1, 0)
        carried = jnp.where(
            group == 0, pltpu.roll(below, nx - wrap_by, 1), pltpu.roll(below, width, 1)
        )
        total = total + jnp.where(sub == 0, carried, below)
        above = pltpu.roll(v, SUB - 1, 0)
        carried = jnp.where(
            group == ztiles - 1, pltpu.roll(above, wrap_by, 1), pltpu.roll(above, nx - width, 1)
        )
        total = total + jnp.where(sub == SUB - 1, carried, above)
        return v, total + (f[e - 1] + f[e + 1])

    @planes(1, ny + 2 * h - 1, DEEP)
    def _(e):
        v, total = around_strip(strip, e)
        rhs_s[e] = 6.0 * v - total

    @planes(2, ny + 2 * h - 2, DEEP)
    def _(e):
        v, total = around_strip(rhs_s, e)
        it_s[e] = alpha * v + beta * total

    def last_strips(e):
        v, total = around_strip(it_s, e)
        u = last_step(v, total, rhs_s[e])
        u = jnp.where(inner < h, pltpu.roll(u, nx - 4 * h, 1), u)
        for zt in range(nz // SUB):
            faces[e, zt * SUB:(zt + 1) * SUB, :] = pltpu.roll(u, (-(width * zt + h)) % nx, 1)

    planes(h, ny + h, DEEP)(last_strips)

    flat_final = final.reshape((ny + 2 * h) * zp, nx)
    flat_faces = faces.reshape((ny + 2 * h) * zp, nx)

    @pl.loop(0, nz // 4)
    def _(block):
        for r in range(4):
            z = block * 4 + r
            for t in range(tiles):
                rows = pl.ds((h + t * SUB) * zp + z, SUB, stride=zp)
                u = jnp.where(edge, flat_faces[rows, :], flat_final[rows, :])
                out[z, t * SUB:(t + 1) * SUB, :] = out[z, t * SUB:(t + 1) * SUB, :] + u

    for k in range(len(offsets)):
        gram_copy(k, me).wait_send()


def hand_over(mixed, weights, out, wout, sem):
    pieces = sem.shape[0]
    per = mixed.shape[0] // pieces
    copies = []
    for c in range(pieces):
        part = pl.ds(c * per, per)
        cp = pltpu.make_async_copy(mixed.at[part], out.at[part], sem.at[c])
        cp.start()
        copies.append(cp)
    wout[...] = weights[...]
    for cp in copies:
        cp.wait()


def on_device(counts, densities, residuals):
    dims = residuals.shape
    count, nz, ny, nx = dims
    h = SWEEPS
    zp = nz + SUB
    n = counts[0] * counts[1] * counts[2]
    chunks = 4
    field = pltpu.VMEM((ny + 2 * h, zp, nx), jnp.float32)
    strips = pltpu.VMEM((ny + 2 * h, SUB, nx), jnp.float32)
    each = 6
    messages = pl.cdiv(ny, each)
    dma = pltpu.SemaphoreType.DMA

    def faces(blocks):
        return pltpu.VMEM((2, blocks, SUB, nx), jnp.float32)

    any_spec = pl.BlockSpec(memory_space=pl.ANY)
    vmem = pl.BlockSpec(memory_space=pltpu.VMEM)
    new_density, weights = pl.pallas_call(
        functools.partial(kernel, counts, dims, chunks),
        out_shape=(
            pltpu.VMEM((nz, ny, nx), jnp.float32),
            pltpu.VMEM((1, count), jnp.float32),
        ),
        in_specs=[any_spec, any_spec],
        out_specs=(vmem, vmem),
        scratch_shapes=[
            pltpu.VMEM((count, nz + 2 * h, ny, nx), jnp.float32),
            pltpu.VMEM(dims, jnp.float32),
            pltpu.VMEM((n, 1, nx), jnp.float32),
            field, field, field, field, field, strips, strips, strips,
            faces(messages),
            faces(messages),
            faces(pl.cdiv(h, each)),
            faces(messages - (ny - h) // each),
            dma((chunks,)), dma(()), dma((n,)), dma((n,)),
            dma((2,)), dma((2,)), dma((2,)), dma((2,)), dma((2,)), dma((2,)), dma((2, 2)), dma((2, 2)),
        ],
        compiler_params=pltpu.CompilerParams(
            collective_id=0, has_side_effects=True, vmem_limit_bytes=61 * 1024 * 1024
        ),
    )(residuals, densities)
    new_density, weights = pl.pallas_call(
        hand_over,
        out_shape=(
            jax.ShapeDtypeStruct((nz, ny, nx), jnp.float32),
            jax.ShapeDtypeStruct((1, count), jnp.float32),
        ),
        in_specs=[vmem, vmem],
        out_specs=(any_spec, vmem),
        scratch_shapes=[dma((4,))],
        compiler_params=pltpu.CompilerParams(vmem_limit_bytes=4 * 1024 * 1024),
    )(new_density, weights)
    return new_density, weights.reshape(count)


def solution(mesh):
    counts = tuple(mesh.shape[a] for a in AXES)
    placed = (P(None, "gz", "gy", "gx"), P(None, "gz", "gy", "gx"))
    return jax.shard_map(
        functools.partial(on_device, counts),
        mesh=mesh,
        in_specs=placed,
        out_specs=(P("gz", "gy", "gx"), P()),
        check_vma=False,
    )
```
